32 devices in a mesh: dp: 4 (over y, x), tensor: 8 (over z, core).
Axes of the slice: x: 2, y: 2, z: 4, core: 2. Of those that a mesh axis runs over, the one named last changes fastest.
Arguments:
- tokens: bfloat16 [768, 4096], P(('dp', 'tensor')), may hold values from -6 to 6
- out_grad: bfloat16 [768, 4096], P(('dp', 'tensor')), may hold values from -6 to 6
- w_gate: bfloat16 [4096, 14336], P(None, 'tensor'), may hold values from -0.09375 to 0.09375
- w_up: bfloat16 [4096, 14336], P(None, 'tensor'), may hold values from -0.09375 to 0.09375
- w_down: bfloat16 [14336, 4096], P('tensor'), may hold values from -0.046875 to 0.046875
Outputs:
- grad_tokens: bfloat16 [768, 4096], P(('dp', 'tensor'))
- grad_gate: bfloat16 [4096, 14336], P('dp', 'tensor')
- grad_up: bfloat16 [4096, 14336], P('dp', 'tensor')
- grad_down: bfloat16 [14336, 4096], P('tensor', 'dp')
The draws below stay inside these ranges and needn't reach their ends.
All inputs are finite; a program needn't handle non-finite values.
Results may differ from the reference program's by a relative error of at most 0.014.
Values may be sent and summed in bfloat16 or wider, within the bound.
No kernel may reach another device: no remote copies, remote signals or barrier semaphores. Data moves between devices by JAX's collectives and lax.ppermute only.
A program may use at most 128 MiB of HBM per device.

```python
import jax
import jax.numpy as jnp
from jax import lax

D = 4096
FF = 14336
TOKENS = 768
N_DP = 4


def block_scale(own_key, shape, shards, least, top_value):
    def one(position, shards_of):
        heights = jax.random.uniform(jax.random.fold_in(jax.random.fold_in(own_key, 6), position), (shards_of,), jnp.float32, least / len(shards), top_value / len(shards))
        return jnp.repeat(jnp.exp(heights), shape[position] // shards_of).reshape((-1,) + (1,) * (len(shape) - position - 1))

    level = one(*shards[0])
    for cut in shards[1:]:
        level = level * one(*cut)
    return level


def noise(key, dims, deviation, most, cuts=(), dtype=jnp.bfloat16):
    values = jax.random.normal(key, dims, jnp.float32) * deviation
    if len(cuts) > 0:
        values = block_scale(key, dims, cuts, -0.22, 0.18) * values
    return jnp.clip(values, min=-most, max=most).astype(dtype)


def setup_inputs(seed: int = 0) -> dict:
    key_list = jax.random.split(jax.random.key(seed), 6)
    tokens = noise(key_list[0], (TOKENS, D), 1.0, 6.0, ((0, 32),))
    out_grad = noise(key_list[1], (TOKENS, D), 1.0, 6.0, ((0, 32),))
    w_gate = noise(key_list[2], (D, FF), D ** -0.5, 0.09375, ((1, 8),))
    w_up = noise(key_list[3], (D, FF), D ** -0.5, 0.09375, ((1, 8),))
    w_down = noise(key_list[4], (FF, D), FF ** -0.5, 0.046875, ((0, 8),))
    return dict(tokens=tokens, out_grad=out_grad, w_gate=w_gate, w_up=w_up, w_down=w_down)


def reference(tokens, out_grad, w_gate, w_up, w_down):
    gate_val = jnp.dot(tokens, w_gate, preferred_element_type=jnp.float32)
    up_val = jnp.dot(tokens, w_up, preferred_element_type=jnp.float32)
    sigmoid_gate = jax.nn.sigmoid(gate_val)
    act_val = gate_val * sigmoid_gate
    hidden = (act_val * up_val).astype(jnp.bfloat16)
    grad_hidden = jnp.dot(out_grad, w_down.T, preferred_element_type=jnp.float32)
    grad_gate_pre = (grad_hidden * up_val * sigmoid_gate * (1.0 + gate_val * (1.0 - sigmoid_gate))).astype(jnp.bfloat16)
    grad_up_pre = (grad_hidden * act_val).astype(jnp.bfloat16)
    grad_tokens = (jnp.dot(grad_gate_pre, w_gate.T, preferred_element_type=jnp.float32)
                   + jnp.dot(grad_up_pre, w_up.T, preferred_element_type=jnp.float32)).astype(jnp.bfloat16)
    token_groups = tokens.reshape(N_DP, -1, D)
    grad_groups = out_grad.reshape(N_DP, -1, D)
    hidden_groups = hidden.reshape(N_DP, -1, FF)
    gate_groups = grad_gate_pre.reshape(N_DP, -1, FF)
    up_groups = grad_up_pre.reshape(N_DP, -1, FF)

    def rounded_add(total, left, right):
        partial_sum = jnp.dot(left.T, right, preferred_element_type=jnp.float32).astype(jnp.bfloat16)
        partial_sum = lax.optimization_barrier(partial_sum)
        return total + partial_sum.astype(jnp.float32)

    def one_group(carried, pieces):
        tok_g, grad_g, hid_g, gate_g, up_g = pieces
        sum_gate, sum_up, sum_down = carried
        return (rounded_add(sum_gate, tok_g, gate_g), rounded_add(sum_up, tok_g, up_g),
                rounded_add(sum_down, hid_g, grad_g)), None

    initial = (jnp.zeros((D, FF), jnp.float32), jnp.zeros((D, FF), jnp.float32), jnp.zeros((FF, D), jnp.float32))
    totals, unused = lax.scan(one_group, initial, (token_groups, grad_groups, hidden_groups, gate_groups, up_groups))
    return (grad_tokens, totals[0].astype(jnp.bfloat16), totals[1].astype(jnp.bfloat16),
            totals[2].astype(jnp.bfloat16))
```

```python
import jax
import jax.numpy as jnp
from jax import lax
from jax.experimental import pallas as pl
from jax.experimental.pallas import tpu as pltpu
from jax.sharding import PartitionSpec as P


def contract_last(left, right):
    return lax.dot_general(
        left, right, (((1,), (1,)), ((), ())), preferred_element_type=jnp.float32
    )


def contract_first(left, right):
    return lax.dot_general(
        left, right, (((0,), (0,)), ((), ())), preferred_element_type=jnp.float32
    )


def stack_rows(pieces):
    count = len(pieces)
    starts = [sum(p.shape[0] for p in pieces[:i]) for i in range(count)]
    total = sum(p.shape[0] for p in pieces)

    def body(*refs):
        out, held, sems_in, sems_out = refs[count:]
        spans = [pl.ds(starts[i], pieces[i].shape[0]) for i in range(count)]
        loads = [
            pltpu.make_async_copy(refs[i], held.at[spans[i]], sems_in.at[i]) for i in range(count)
        ]
        stores = [
            pltpu.make_async_copy(held.at[spans[i]], out.at[spans[i]], sems_out.at[i])
            for i in range(count)
        ]
        for load in loads:
            load.start()
        for load, store in zip(loads, stores):
            load.wait()
            store.start()
        for store in stores:
            store.wait()

    shape = (total, pieces[0].shape[1])
    return pl.pallas_call(
        body,
        out_shape=jax.ShapeDtypeStruct(shape, pieces[0].dtype),
        in_specs=[pl.BlockSpec(memory_space=pl.ANY)] * count,
        out_specs=pl.BlockSpec(memory_space=pl.ANY),
        scratch_shapes=[
            pltpu.VMEM(shape, pieces[0].dtype),
            pltpu.SemaphoreType.DMA((count,)),
            pltpu.SemaphoreType.DMA((count,)),
        ],
        name="stack_rows",
    )(*pieces)


def input_terms(dgate, dup, w_gate, w_up):
    rows, units = dgate.shape
    width = w_gate.shape[0]
    block = min(512, width)

    def body(dgate_ref, dup_ref, gate_ref, up_ref, out_ref):
        total = contract_last(gate_ref[...], dgate_ref[...]) + contract_last(
            up_ref[...], dup_ref[...]
        )
        out_ref[...] = total.T

    whole = pl.BlockSpec((rows, units), lambda i: (0, 0))
    part = pl.BlockSpec((block, units), lambda i: (i, 0))
    return pl.pallas_call(
        body,
        grid=(width // block,),
        out_shape=jax.ShapeDtypeStruct((rows, width), jnp.float32),
        in_specs=[whole, whole, part, part],
        out_specs=pl.BlockSpec((rows, block), lambda i: (0, i)),
        cost_estimate=pl.CostEstimate(
            flops=4 * rows * units * width, bytes_accessed=4 * units * width, transcendentals=0
        ),
        name="input_terms",
    )(dgate, dup, w_gate, w_up)


def swap(value, axis, mask):
    size = lax.axis_size(axis)
    return lax.ppermute(value, axis, [(i, i ^ mask) for i in range(size)])


def own_half(rows):
    pieces = [rows]
    for step in range(1, lax.axis_size("tensor") // 2):
        pieces.append(swap(rows, "tensor", 2 * step))
    return jnp.concatenate(pieces, axis=0)


def exchange(sides, first, last):
    groups = lax.axis_size("dp")
    bits = [1 << k for k in range(groups.bit_length() - 1)]
    done = []
    for held, order in zip(sides, (bits, bits[::-1])):
        held = dict(held)
        for bit in order[first:last]:
            for offset, value in list(held.items()):
                held[offset ^ bit] = swap(value, "dp", bit)
        done.append(held)
    return done


def quarters(half):
    cut = half.shape[0] // 2
    return [{0: half[:cut]}, {0: half[cut:]}]


def other_pieces(sides):
    mine = [side[g] for g in range(1, lax.axis_size("dp")) for side in sides]
    return mine + [swap(piece, "tensor", 1) for piece in mine]


def forward(tokens, w_gate, w_up):
    gate_val = jnp.dot(tokens, w_gate, preferred_element_type=jnp.float32)
    up_val = jnp.dot(tokens, w_up, preferred_element_type=jnp.float32)
    return gate_val, up_val


def hidden_terms(gate_val, up_val, grads, w_down):
    sigmoid_gate = jax.nn.sigmoid(gate_val)
    act_val = gate_val * sigmoid_gate
    hidden = (act_val * up_val).astype(jnp.bfloat16)
    grad_hidden = contract_last(grads, w_down)
    grad_gate_pre = (
        grad_hidden * up_val * sigmoid_gate * (1.0 + gate_val * (1.0 - sigmoid_gate))
    ).astype(jnp.bfloat16)
    grad_up_pre = (grad_hidden * act_val).astype(jnp.bfloat16)
    return hidden, grad_gate_pre, grad_up_pre


def finish_sum(partial, from_core, rows):
    chip = partial[: partial.shape[0] // 2] + from_core.astype(jnp.float32)
    total = chip[:rows]
    for step in range(1, lax.axis_size("tensor") // 2):
        piece = chip[step * rows : (step + 1) * rows].astype(jnp.bfloat16)
        total = total + swap(piece, "tensor", 2 * step).astype(jnp.float32)
    return total.astype(jnp.bfloat16)


def per_device(tokens, out_grad, w_gate, w_up, w_down):
    tie = lax.optimization_barrier
    group = lax.axis_index("dp")
    col_width = tokens.shape[1] // lax.axis_size("dp")
    stages = lax.axis_size("dp").bit_length() - 1
    tok_half = own_half(tokens)
    tok_half, out_grad = tie((tok_half, out_grad))
    grad_half = own_half(out_grad)

    tok_other, tok_half = tie((swap(tok_half, "tensor", 1), tok_half))
    own_tokens = jnp.concatenate([tok_half, tok_other], axis=0)
    tok_sides = exchange(quarters(tok_half), 0, 1)
    own_gate, own_up = forward(own_tokens, w_gate, w_up)
    tok_sides, grad_half, own_gate, own_up = tie((tok_sides, grad_half, own_gate, own_up))

    grad_other, grad_half, tok_sides = tie((swap(grad_half, "tensor", 1), grad_half, tok_sides))
    own_grads = jnp.concatenate([grad_half, grad_other], axis=0)
    tok_sides = exchange(tok_sides, 1, stages)
    grad_sides = exchange(quarters(grad_half), 0, 1)
    own_hidden, own_dgate, own_dup = hidden_terms(own_gate, own_up, own_grads, w_down)
    own_hidden, own_dgate, own_dup, tok_first = tie((own_hidden, own_dgate, own_dup, tok_sides))
    tok_sides = tok_first

    rest_list = other_pieces(tok_sides)
    grad_sides = exchange(grad_sides, 1, stages)
    partial = input_terms(own_dgate, own_dup, w_gate, w_up)
    partial, rest_list = tie((partial, rest_list))
    from_core = swap(partial[partial.shape[0] // 2 :].astype(jnp.bfloat16), "tensor", 1)
    rest_tokens = stack_rows(rest_list)
    rest_gate = jnp.dot(rest_tokens, w_gate, preferred_element_type=jnp.float32)
    rest_gate, rest_tokens, grad_sides, from_core = tie((rest_gate, rest_tokens, grad_sides, from_core))
    grad_tokens = finish_sum(partial, from_core, tokens.shape[0])
    grad_list = other_pieces(grad_sides)
    rest_up = jnp.dot(rest_tokens, w_up, preferred_element_type=jnp.float32)
    rest_up, rest_tokens, grad_list = tie((rest_up, rest_tokens, grad_list))
    rest_grads = stack_rows(grad_list)
    rest_hidden, rest_dgate, rest_dup = hidden_terms(rest_gate, rest_up, rest_grads, w_down)

    def columns(own, rest):
        return jnp.concatenate(
            [lax.dynamic_slice_in_dim(a, group * col_width, col_width, 1) for a in (own, rest)], axis=0
        )

    tok_cols = columns(own_tokens, rest_tokens)
    grad_cols = columns(own_grads, rest_grads)
    hidden = jnp.concatenate([own_hidden, rest_hidden], axis=0)
    dgate = jnp.concatenate([own_dgate, rest_dgate], axis=0)
    dup = jnp.concatenate([own_dup, rest_dup], axis=0)
    return (
        grad_tokens,
        contract_first(tok_cols, dgate).astype(jnp.bfloat16),
        contract_first(tok_cols, dup).astype(jnp.bfloat16),
        contract_first(hidden, grad_cols).astype(jnp.bfloat16),
    )


def solution(mesh):
    in_specs = (
        P(("dp", "tensor"), None),
        P(("dp", "tensor"), None),
        P(None, "tensor"),
        P(None, "tensor"),
        P("tensor", None),
    )
    out_specs = (P(("dp", "tensor"), None), P("dp", "tensor"), P("dp", "tensor"), P("tensor", "dp"))
    return jax.shard_map(
        per_device, mesh=mesh, in_specs=in_specs, out_specs=out_specs, check_vma=False
    )
```
